32 devices in a mesh: row: 16 (over z, y, core), col: 2 (over x).
Axes of the slice: x: 2, y: 2, z: 4, core: 2. Of those that a mesh axis runs over, the one named last changes fastest.
Arguments:
- left: bfloat16 [16384, 16384], P('row', 'col'), may hold values from -6 to 6
- right: bfloat16 [16384, 16384], P('row', 'col'), may hold values from -0.09375 to 0.09375
Outputs:
- product: bfloat16 [16384, 16384], P('row', 'col')
The draws below stay inside these ranges and needn't reach their ends.
All inputs are finite; a program needn't handle non-finite values.
Results may differ from the reference program's by a relative error of at most 0.001.
Values may be sent and summed in bfloat16 or wider, within the bound.
A program may use at most 256 MiB of HBM per device.

```python
import jax
import jax.numpy as jnp
from jax import lax

N = 16384
STEPS = 4
GRID = 16
KB = 1024


def steps_of(stream_key, shape, split, least, largest):
    factor_of, own = 1.0, jax.random.fold_in(stream_key, 6)
    for axis_at, shards_of in split:
        steps = jnp.exp(jax.random.uniform(jax.random.fold_in(own, axis_at), (shards_of,), jnp.float32, least / len(split), largest / len(split)))
        factor_of = factor_of * jnp.repeat(steps, shape[axis_at] // shards_of).reshape([-1 if axis == axis_at else 1 for axis in range(len(shape))])
    return factor_of


def scatter_about(rng, extent, spread, bound, split=(), kind=jnp.bfloat16):
    result = jax.random.normal(rng, extent, jnp.float32) * spread
    if len(split) > 0:
        result = steps_of(rng, extent, split, -0.22, 0.18) * result
    return jnp.clip(result, min=-bound, max=bound).astype(kind)


def setup_inputs(seed: int = 0) -> dict:
    key_list = jax.random.split(jax.random.key(seed), 3)
    return {
        "left": scatter_about(key_list[0], (N, N), 1.0, 6.0, ((0, 16), (1, 2))),
        "right": scatter_about(key_list[1], (N, N), (STEPS * KB) ** -0.5, 0.09375, ((0, 16), (1, 2))),
    }


def reference(left, right):
    def block_row(index):
        total = jnp.zeros((KB, N), jnp.float32)
        for offset in range(STEPS):
            kblock = (index + offset) % GRID
            piece = lax.dynamic_slice(left, (index * KB, kblock * KB), (KB, KB))
            rows = lax.dynamic_slice_in_dim(right, kblock * KB, KB, 0)
            total = total + jnp.dot(piece, rows, preferred_element_type=jnp.float32)
        return total.astype(jnp.bfloat16)

    blocks = lax.map(block_row, jnp.arange(GRID, dtype=jnp.int32))
    return blocks.reshape(N, N)
```

```python
import functools

import jax
import jax.numpy as jnp
from jax import lax
from jax.experimental import pallas as pl
from jax.experimental.pallas import tpu as pltpu
from jax.sharding import PartitionSpec as P

STEPS = 4
WIDTH = 256
AHEAD = 6
BURST = 3
MESH = pl.DeviceIdType.MESH


def kernel(grid_rows, col_count, width, start, left, right, out, arr_a, arr_b, arr_z, arr_d,
           lbuf, rbuf, obuf, sem_a, sem_b, sem_z, sem_d, send, lsend, lrecv, load_sem, out_sem):
    row = lax.axis_index("row")
    col = lax.axis_index("col")
    rows, columns = right.shape
    chunks = columns // width
    per_shard = grid_rows // col_count
    c = row % 2
    p = (row // 2) % 2
    group = row - 2 * p - c
    partner = group + 2 * p + 1 - c
    across = group + 2 * (1 - p) + c
    z_to = (row + grid_rows - 3 - 2 * c) % grid_rows
    z_from = (row + 5 - 2 * c) % grid_rows

    barrier = pltpu.get_barrier_semaphore()
    for other in (partner, across, z_to, z_from):
        pl.semaphore_signal(barrier, inc=1, device_id={"row": other}, device_id_type=MESH)
    for step in range(1, col_count):
        pl.semaphore_signal(barrier, inc=1, device_id={"col": (col + step) % col_count}, device_id_type=MESH)
    pl.semaphore_wait(barrier, 4 + col_count - 1)

    def cut(ref, j):
        return ref.at[:, pl.ds(pl.multiple_of(j * width, width), width)]

    def remote(src, dst, j, which, recv, to):
        return pltpu.make_async_remote_copy(
            src_ref=cut(src, j), dst_ref=cut(dst, j), send_sem=send.at[which],
            recv_sem=recv.at[j], device_id={"row": to}, device_id_type=MESH)

    def arrival(dst, recv, j):
        pltpu.make_async_copy(cut(dst, j), cut(dst, j), recv.at[j]).wait()

    has_z_out = (p * c) == 0
    has_z_in = ((1 - p) + c) > 0

    def send_own(j):
        @pl.when(p == 1)
        def _():
            remote(right, arr_a, j, 0, sem_a, across).start()

        @pl.when(has_z_out)
        def _():
            remote(right, arr_z, j, 1, sem_z, z_to).start()

        @pl.when(c == 1)
        def _():
            remote(right, arr_d, j, 2, sem_d, partner).start()

    turns = (0, 2 + p * (1 - 2 * c), 2 + (1 - p) * (1 - 2 * c), 1 + 2 * c)

    def left_of(t):
        block = (row + turns[t]) % grid_rows
        source = left.at[:, pl.ds(pl.multiple_of(block % per_shard * rows, rows), rows)]
        slot = lbuf.at[:, pl.ds(t * rows, rows)]
        return block // per_shard, source, slot

    def left_copy(t, step):
        _, source, slot = left_of(t)
        return pltpu.make_async_remote_copy(
            src_ref=source, dst_ref=slot, send_sem=lsend.at[t, step - 1], recv_sem=lrecv.at[t],
            device_id={"col": (col + step) % col_count}, device_id_type=MESH)

    ahead = min(AHEAD, chunks)

    def first(j, _):
        send_own(j)
        return 0

    lax.fori_loop(0, ahead, first, 0)
    for t in range(STEPS):
        owner, source, slot = left_of(t)

        @pl.when(owner == col)
        def _():
            for step in range(1, col_count):
                left_copy(t, step).start()
            pltpu.make_async_copy(source, slot, lrecv.at[t]).start()

    def relay(i):
        @pl.when(i + ahead < chunks)
        def _():
            send_own(i + ahead)

        @pl.when(has_z_in)
        def _():
            arrival(arr_z, sem_z, i)

            @pl.when(p == 0)
            def _():
                remote(arr_z, arr_a, i, 4, sem_a, across).start()

        arrival(arr_a, sem_a, i)
        remote(arr_a, arr_b, i, 3, sem_b, partner).start()

    def load(src, j, slot, t):
        return pltpu.make_async_copy(
            cut(src, j), rbuf.at[slot, pl.ds(t * rows, rows), :], load_sem.at[slot, t])

    def store(j, slot):
        return pltpu.make_async_copy(obuf.at[slot], cut(out, j), out_sem.at[slot])

    def compute(first_chunk, count):
        for n in range(count):
            j = first_chunk + n
            arrival(arr_b, sem_b, j)
            load(right, j, n, 0).start()
            load(arr_a, j, n, 1).start()
            load(arr_b, j, n, 2).start()

            @pl.when(c == 0)
            def _():
                arrival(arr_d, sem_d, j)
                load(arr_d, j, n, 3).start()

            @pl.when(c == 1)
            def _():
                load(arr_z, j, n, 3).start()

        def one(n, _):
            for t in range(STEPS):
                load(right, first_chunk + n, n, t).wait()
            obuf[n] = jnp.dot(lbuf[...], rbuf[n], preferred_element_type=jnp.float32).astype(obuf.dtype)
            store(first_chunk + n, n).start()
            return 0

        lax.fori_loop(0, count, one, 0)
        for n in range(count):
            store(first_chunk + n, n).wait()

    def only_relay(i, _):
        relay(i)
        return 0

    lax.fori_loop(0, start, only_relay, 0)
    for t in range(STEPS):
        pltpu.make_async_copy(left_of(t)[2], left_of(t)[2], lrecv.at[t]).wait()

    def burst(i, _):
        relay(i)
        compute((i - start) * BURST, BURST)
        return 0

    caught = start + start // (BURST - 1)
    lax.fori_loop(start, caught, burst, 0)

    def level(i, _):
        relay(i)
        compute(i, 1)
        return 0

    lax.fori_loop(caught, chunks, level, 0)

    def sent(which):
        pltpu.make_async_copy(right, right, send.at[which]).wait()

    @pl.when(p == 1)
    def _():
        sent(0)

    @pl.when(has_z_out)
    def _():
        sent(1)

    @pl.when(c == 1)
    def _():
        sent(2)

    sent(3)

    @pl.when(p == 0)
    def _():
        sent(4)

    for t in range(STEPS):
        @pl.when(left_of(t)[0] == col)
        def _():
            for step in range(1, col_count):
                left_copy(t, step).wait_send()


def solution(mesh):
    grid_rows, col_count = mesh.shape["row"], mesh.shape["col"]

    def local(left, right):
        rows, columns = right.shape
        width = min(WIDTH, columns // 8)
        chunks = columns // width
        start = (chunks * 9 // 16) // 2 * 2
        block = jax.ShapeDtypeStruct((rows, columns), jnp.bfloat16)
        dma = pltpu.SemaphoreType.DMA
        results = pl.pallas_call(
            functools.partial(kernel, grid_rows, col_count, width, start),
            out_shape=[block] * 5,
            in_specs=[pl.BlockSpec(memory_space=pl.ANY)] * 2,
            out_specs=[pl.BlockSpec(memory_space=pl.ANY)] * 5,
            scratch_shapes=[
                pltpu.VMEM((rows, STEPS * rows), jnp.bfloat16),
                pltpu.VMEM((BURST, STEPS * rows, width), jnp.bfloat16),
                pltpu.VMEM((BURST, rows, width), jnp.bfloat16),
                dma((chunks,)), dma((chunks,)), dma((chunks,)), dma((chunks,)),
                dma((5,)), dma((STEPS, col_count - 1)), dma((STEPS,)),
                dma((BURST, STEPS)), dma((BURST,)),
            ],
            compiler_params=pltpu.CompilerParams(
                collective_id=0, has_side_effects=True, vmem_limit_bytes=60 * 1024 * 1024),
        )(left, right)
        return results[0]

    return jax.shard_map(
        local,
        mesh=mesh,
        in_specs=(P("row", "col"), P("row", "col")),
        out_specs=P("row", "col"),
        check_vma=False,
    )
```

```python
import functools

import jax
import jax.numpy as jnp
from jax import lax
from jax.experimental import pallas as pl
from jax.experimental.pallas import tpu as pltpu
from jax.sharding import PartitionSpec as P

STEPS = 4
WIDTH = 256
AHEAD = 6
BURST = 3
EARLY = 3
MESH = pl.DeviceIdType.MESH


def kernel(grid_rows, col_count, width, start, left, right, out, arr_a, arr_b, arr_z, arr_d,
           lbuf, rbuf, sem_a, sem_b, sem_z, sem_d, send, lsend, lrecv, load_sem):
    row = lax.axis_index("row")
    col = lax.axis_index("col")
    rows, columns = right.shape
    chunks = columns // width
    per_shard = grid_rows // col_count
    c = row % 2
    p = (row // 2) % 2
    group = row - 2 * p - c
    partner = group + 2 * p + 1 - c
    across = group + 2 * (1 - p) + c
    z_to = (row + grid_rows - 3 - 2 * c) % grid_rows
    z_from = (row + 5 - 2 * c) % grid_rows

    barrier = pltpu.get_barrier_semaphore()
    for other in (partner, across, z_to, z_from):
        pl.semaphore_signal(barrier, inc=1, device_id={"row": other}, device_id_type=MESH)
    for step in range(1, col_count):
        pl.semaphore_signal(barrier, inc=1, device_id={"col": (col + step) % col_count}, device_id_type=MESH)
    pl.semaphore_wait(barrier, 4 + col_count - 1)

    def cut(ref, j):
        return ref.at[:, pl.ds(pl.multiple_of(j * width, width), width)]

    def remote(src, dst, j, which, recv, to):
        return pltpu.make_async_remote_copy(
            src_ref=cut(src, j), dst_ref=cut(dst, j), send_sem=send.at[which],
            recv_sem=recv.at[j], device_id={"row": to}, device_id_type=MESH)

    def arrival(dst, recv, j):
        pltpu.make_async_copy(cut(dst, j), cut(dst, j), recv.at[j]).wait()

    has_z_out = (p * c) == 0
    has_z_in = ((1 - p) + c) > 0

    odd_low = (1 - p) * c == 1
    odd_high = p * c == 1

    def send_own(j):
        @pl.when(odd_low & (j < EARLY))
        def _():
            remote(right, arr_d, j, 5, sem_d, across).start()

        @pl.when(p == 1)
        def _():
            remote(right, arr_a, j, 0, sem_a, across).start()

        @pl.when(has_z_out & ((c == 0) | (j >= EARLY)))
        def _():
            remote(right, arr_z, j, 1, sem_z, z_to).start()

        @pl.when(c == 1)
        def _():
            remote(right, arr_d, j, 2, sem_d, partner).start()

    turns = (0, 2 + p * (1 - 2 * c), 2 + (1 - p) * (1 - 2 * c), 1 + 2 * c)

    def left_of(t):
        block = (row + turns[t]) % grid_rows
        source = left.at[:, pl.ds(pl.multiple_of(block % per_shard * rows, rows), rows)]
        slot = lbuf.at[:, pl.ds(t * rows, rows)]
        return block // per_shard, source, slot

    def left_copy(t, step):
        _, source, slot = left_of(t)
        return pltpu.make_async_remote_copy(
            src_ref=source, dst_ref=slot, send_sem=lsend.at[t, step - 1], recv_sem=lrecv.at[t],
            device_id={"col": (col + step) % col_count}, device_id_type=MESH)

    ahead = min(AHEAD, chunks)

    def first(j, _):
        send_own(j)
        return 0

    lax.fori_loop(0, ahead, first, 0)
    for t in range(STEPS):
        owner, source, slot = left_of(t)

        @pl.when(owner == col)
        def _():
            for step in range(1, col_count):
                left_copy(t, step).start()
            pltpu.make_async_copy(source, slot, lrecv.at[t]).start()

    def relay(i):
        @pl.when(i + ahead < chunks)
        def _():
            send_own(i + ahead)

        @pl.when(odd_high & (i < EARLY))
        def _():
            arrival(arr_d, sem_d, i)
            remote(arr_d, arr_a, i, 6, sem_a, z_to).start()

        @pl.when(has_z_in & ((c == 1) | (i >= EARLY)))
        def _():
            arrival(arr_z, sem_z, i)

            @pl.when(p == 0)
            def _():
                remote(arr_z, arr_a, i, 4, sem_a, across).start()

        arrival(arr_a, sem_a, i)
        remote(arr_a, arr_b, i, 3, sem_b, partner).start()

    def load(src, j, slot, t):
        return pltpu.make_async_copy(
            cut(src, j), rbuf.at[slot, pl.ds(t * rows, rows), :], load_sem.at[slot, t])

    def compute(first_chunk, count):
        for n in range(count):
            j = first_chunk + n
            arrival(arr_b, sem_b, j)
            load(right, j, n, 0).start()
            load(arr_a, j, n, 1).start()
            load(arr_b, j, n, 2).start()

            @pl.when(c == 0)
            def _():
                arrival(arr_d, sem_d, j)
                load(arr_d, j, n, 3).start()

            @pl.when(c == 1)
            def _():
                load(arr_z, j, n, 3).start()

        def one(n, _):
            for t in range(STEPS):
                load(right, first_chunk + n, n, t).wait()
            out[first_chunk + n] = jnp.dot(
                lbuf[...], rbuf[n], preferred_element_type=jnp.float32).astype(out.dtype)
            return 0

        lax.fori_loop(0, count, one, 0)

    def only_relay(i, _):
        relay(i)
        return 0

    lax.fori_loop(0, start, only_relay, 0)
    for t in range(STEPS):
        pltpu.make_async_copy(left_of(t)[2], left_of(t)[2], lrecv.at[t]).wait()

    def burst(i, _):
        relay(i)
        compute((i - start) * BURST, BURST)
        return 0

    caught = start + start // (BURST - 1)
    lax.fori_loop(start, caught, burst, 0)

    def level(i, _):
        relay(i)
        compute(i, 1)
        return 0

    lax.fori_loop(caught, chunks, level, 0)

    def sent(which, begin=0, end=chunks):
        part = right.at[:, pl.ds(begin * width, (end - begin) * width)]
        pltpu.make_async_copy(part, part, send.at[which]).wait()

    @pl.when(p == 1)
    def _():
        sent(0)

    @pl.when(c == 0)
    def _():
        sent(1)

    @pl.when(odd_low)
    def _():
        sent(1, EARLY)
        sent(5, 0, EARLY)

    @pl.when(odd_high)
    def _():
        sent(6, 0, EARLY)

    @pl.when(c == 1)
    def _():
        sent(2)

    sent(3)

    @pl.when((p + c) == 0)
    def _():
        sent(4, EARLY)

    @pl.when(odd_low)
    def _():
        sent(4)

    for t in range(STEPS):
        @pl.when(left_of(t)[0] == col)
        def _():
            for step in range(1, col_count):
                left_copy(t, step).wait_send()


def write(chunks, width, held, out, sem):
    def copy(j):
        place = pl.ds(pl.multiple_of(j * width, width), width)
        return pltpu.make_async_copy(held.at[j], out.at[:, place], sem.at[j])

    for j in range(chunks):
        copy(j).start()
    for j in range(chunks):
        copy(j).wait()


def solution(mesh):
    grid_rows, col_count = mesh.shape["row"], mesh.shape["col"]

    def local(left, right):
        rows, columns = right.shape
        width = min(WIDTH, columns // 8)
        chunks = columns // width
        start = (chunks * 9 // 16) // 2 * 2
        block = jax.ShapeDtypeStruct((rows, columns), jnp.bfloat16)
        dma = pltpu.SemaphoreType.DMA
        results = pl.pallas_call(
            functools.partial(kernel, grid_rows, col_count, width, start),
            out_shape=[pltpu.VMEM((chunks, rows, width), jnp.bfloat16)] + [block] * 4,
            in_specs=[pl.BlockSpec(memory_space=pl.ANY)] * 2,
            out_specs=[pl.BlockSpec(memory_space=pltpu.VMEM)] + [pl.BlockSpec(memory_space=pl.ANY)] * 4,
            scratch_shapes=[
                pltpu.VMEM((rows, STEPS * rows), jnp.bfloat16),
                pltpu.VMEM((BURST, STEPS * rows, width), jnp.bfloat16),
                dma((chunks,)), dma((chunks,)), dma((chunks,)), dma((chunks,)),
                dma((7,)), dma((STEPS, col_count - 1)), dma((STEPS,)),
                dma((BURST, STEPS)),
            ],
            compiler_params=pltpu.CompilerParams(
                collective_id=0, has_side_effects=True, vmem_limit_bytes=40 * 1024 * 1024),
        )(left, right)
        return pl.pallas_call(
            functools.partial(write, chunks, width),
            out_shape=block,
            in_specs=[pl.BlockSpec(memory_space=pltpu.VMEM)],
            out_specs=pl.BlockSpec(memory_space=pl.ANY),
            scratch_shapes=[dma((chunks,))],
            compiler_params=pltpu.CompilerParams(vmem_limit_bytes=20 * 1024 * 1024),
        )(results[0])

    return jax.shard_map(
        local,
        mesh=mesh,
        in_specs=(P("row", "col"), P("row", "col")),
        out_specs=P("row", "col"),
        check_vma=False,
    )
```

```python
import functools

import jax
import jax.numpy as jnp
from jax import lax
from jax.experimental import pallas as pl
from jax.experimental.pallas import tpu as pltpu
from jax.sharding import PartitionSpec as P

STEPS = 4
WIDTH = 256
AHEAD = 6
BURST = 3
EARLY = 3
MESH = pl.DeviceIdType.MESH


def kernel(grid_rows, col_count, width, start, left, right, out, lbuf, arr_a, arr_b, arr_z, arr_d,
           rbuf, sem_a, sem_b, sem_z, sem_d, send, lsend, lrecv, load_sem):
    row = lax.axis_index("row")
    col = lax.axis_index("col")
    rows, columns = right.shape
    chunks = columns // width
    per_shard = grid_rows // col_count
    c = row % 2
    p = (row // 2) % 2
    group = row - 2 * p - c
    partner = group + 2 * p + 1 - c
    across = group + 2 * (1 - p) + c
    z_to = (row + grid_rows - 3 - 2 * c) % grid_rows
    z_from = (row + 5 - 2 * c) % grid_rows

    barrier = pltpu.get_barrier_semaphore()
    for other in (partner, across, z_to, z_from):
        pl.semaphore_signal(barrier, inc=1, device_id={"row": other}, device_id_type=MESH)
    for step in range(1, col_count):
        pl.semaphore_signal(barrier, inc=1, device_id={"col": (col + step) % col_count}, device_id_type=MESH)
    pl.semaphore_wait(barrier, 4 + col_count - 1)

    def cut(ref, j):
        return ref.at[:, pl.ds(pl.multiple_of(j * width, width), width)]

    def remote(src, dst, j, which, recv, to):
        return pltpu.make_async_remote_copy(
            src_ref=cut(src, j), dst_ref=cut(dst, j), send_sem=send.at[which],
            recv_sem=recv.at[j], device_id={"row": to}, device_id_type=MESH)

    def arrival(dst, recv, j):
        pltpu.make_async_copy(cut(dst, j), cut(dst, j), recv.at[j]).wait()

    has_z_out = (p * c) == 0

    odd_low = (1 - p) * c == 1
    odd_high = p * c == 1

    def send_own(j):
        @pl.when(odd_low & (j < EARLY))
        def _():
            remote(right, arr_d, j, 5, sem_d, across).start()

        @pl.when(p == 1)
        def _():
            remote(right, arr_a, j, 0, sem_a, across).start()

        @pl.when(has_z_out & ((c == 0) | (j >= EARLY)))
        def _():
            remote(right, arr_z, j, 1, sem_z, z_to).start()

        @pl.when(c == 1)
        def _():
            remote(right, arr_d, j, 2, sem_d, partner).start()

    turns = (0, 2 + p * (1 - 2 * c), 2 + (1 - p) * (1 - 2 * c), 1 + 2 * c)

    def left_of(t):
        block = (row + turns[t]) % grid_rows
        source = left.at[:, pl.ds(pl.multiple_of(block % per_shard * rows, rows), rows)]
        slot = lbuf.at[:, pl.ds(t * rows, rows)]
        return block // per_shard, source, slot

    def left_copy(t, step):
        _, source, slot = left_of(t)
        return pltpu.make_async_remote_copy(
            src_ref=source, dst_ref=slot, send_sem=lsend.at[t, step - 1], recv_sem=lrecv.at[t],
            device_id={"col": (col + step) % col_count}, device_id_type=MESH)

    ahead = min(AHEAD, chunks)

    def first(j, _):
        send_own(j)
        return 0

    lax.fori_loop(0, ahead, first, 0)
    for t in range(STEPS):
        owner, source, slot = left_of(t)

        @pl.when(owner == col)
        def _():
            for step in range(1, col_count):
                left_copy(t, step).start()
            pltpu.make_async_copy(source, slot, lrecv.at[t]).start()

    def relay(i):
        @pl.when(i + ahead < chunks)
        def _():
            send_own(i + ahead)

        @pl.when(odd_high & (i < EARLY))
        def _():
            arrival(arr_d, sem_d, i)
            remote(arr_d, arr_a, i, 6, sem_a, z_to).start()

        def relay_z(j):
            arrival(arr_z, sem_z, j)

            @pl.when(p == 0)
            def _():
                remote(arr_z, arr_a, j, 4, sem_a, across).start()

        @pl.when(((p + c) == 0) & (i + EARLY < chunks))
        def _():
            relay_z(i + EARLY)

        @pl.when((c == 1) & (i < chunks - 1))
        def _():
            relay_z(i)

        @pl.when((c == 1) & (i == chunks - 2))
        def _():
            relay_z(i + 1)

        arrival(arr_a, sem_a, i)
        remote(arr_a, arr_b, i, 3, sem_b, partner).start()

    def load(src, j, slot, t):
        return pltpu.make_async_copy(
            cut(src, j), rbuf.at[slot, pl.ds(t * rows, rows), :], load_sem.at[slot, t])

    def compute(first_chunk, count):
        for n in range(count):
            j = first_chunk + n
            arrival(arr_b, sem_b, j)
            load(right, j, n, 0).start()
            load(arr_a, j, n, 1).start()
            load(arr_b, j, n, 2).start()

            @pl.when(c == 0)
            def _():
                arrival(arr_d, sem_d, j)
                load(arr_d, j, n, 3).start()

            @pl.when(c == 1)
            def _():
                load(arr_z, j, n, 3).start()

        def one(n, _):
            for t in range(STEPS):
                load(right, first_chunk + n, n, t).wait()
            out[first_chunk + n] = jnp.dot(
                lbuf[...], rbuf[n], preferred_element_type=jnp.float32).astype(out.dtype)
            return 0

        lax.fori_loop(0, count, one, 0)

    def only_relay(i, _):
        relay(i)
        return 0

    lax.fori_loop(0, start, only_relay, 0)
    for t in range(STEPS):
        pltpu.make_async_copy(left_of(t)[2], left_of(t)[2], lrecv.at[t]).wait()

    def burst(i, _):
        relay(i)
        compute((i - start) * BURST, BURST)
        return 0

    caught = start + start // (BURST - 1)
    lax.fori_loop(start, caught, burst, 0)

    def level(i, _):
        relay(i)
        compute(i, 1)
        return 0

    lax.fori_loop(caught, chunks - 1, level, 0)
    relay(chunks - 1)
    arrival(arr_b, sem_b, chunks - 1)

    @pl.when(c == 0)
    def _():
        arrival(arr_d, sem_d, chunks - 1)

    def sent(which, begin=0, end=chunks):
        part = right.at[:, pl.ds(begin * width, (end - begin) * width)]
        pltpu.make_async_copy(part, part, send.at[which]).wait()

    @pl.when(p == 1)
    def _():
        sent(0)

    @pl.when(c == 0)
    def _():
        sent(1)

    @pl.when(odd_low)
    def _():
        sent(1, EARLY)
        sent(5, 0, EARLY)

    @pl.when(odd_high)
    def _():
        sent(6, 0, EARLY)

    @pl.when(c == 1)
    def _():
        sent(2)

    sent(3)

    @pl.when((p + c) == 0)
    def _():
        sent(4, EARLY)

    @pl.when(odd_low)
    def _():
        sent(4)

    for t in range(STEPS):
        @pl.when(left_of(t)[0] == col)
        def _():
            for step in range(1, col_count):
                left_copy(t, step).wait_send()


def write(chunks, width, held, lbuf, right, arr_a, arr_b, arr_z, arr_d, out, rbuf, obuf, sem, load_sem):
    c = lax.axis_index("row") % 2
    rows = right.shape[0]
    last = chunks - 1

    def load(src, t):
        return pltpu.make_async_copy(
            src.at[:, pl.ds(last * width, width)], rbuf.at[pl.ds(t * rows, rows), :], load_sem.at[t])

    load(right, 0).start()
    load(arr_a, 1).start()
    load(arr_b, 2).start()

    @pl.when(c == 0)
    def _():
        load(arr_d, 3).start()

    @pl.when(c == 1)
    def _():
        load(arr_z, 3).start()

    def copy(j):
        src = obuf if j == last else held.at[j]
        return pltpu.make_async_copy(src, out.at[:, pl.ds(j * width, width)], sem.at[j])

    for j in range(last):
        copy(j).start()
    for t in range(STEPS):
        load(right, t).wait()
    obuf[...] = jnp.dot(lbuf[...], rbuf[...], preferred_element_type=jnp.float32).astype(obuf.dtype)
    copy(last).start()
    for j in range(chunks):
        copy(j).wait()


def solution(mesh):
    grid_rows, col_count = mesh.shape["row"], mesh.shape["col"]

    def local(left, right):
        rows, columns = right.shape
        width = min(WIDTH, columns // 8)
        chunks = columns // width
        start = (chunks * 9 // 16) // 2 * 2
        block = jax.ShapeDtypeStruct((rows, columns), jnp.bfloat16)
        dma = pltpu.SemaphoreType.DMA
        results = pl.pallas_call(
            functools.partial(kernel, grid_rows, col_count, width, start),
            out_shape=[
                pltpu.VMEM((chunks - 1, rows, width), jnp.bfloat16),
                pltpu.VMEM((rows, STEPS * rows), jnp.bfloat16),
            ] + [block] * 4,
            in_specs=[pl.BlockSpec(memory_space=pl.ANY)] * 2,
            out_specs=[pl.BlockSpec(memory_space=pltpu.VMEM)] * 2 + [pl.BlockSpec(memory_space=pl.ANY)] * 4,
            scratch_shapes=[
                pltpu.VMEM((BURST, STEPS * rows, width), jnp.bfloat16),
                dma((chunks,)), dma((chunks,)), dma((chunks,)), dma((chunks,)),
                dma((7,)), dma((STEPS, col_count - 1)), dma((STEPS,)),
                dma((BURST, STEPS)),
            ],
            compiler_params=pltpu.CompilerParams(
                collective_id=0, has_side_effects=True, vmem_limit_bytes=30 * 1024 * 1024),
        )(left, right)
        return pl.pallas_call(
            functools.partial(write, chunks, width),
            out_shape=block,
            in_specs=[pl.BlockSpec(memory_space=pltpu.VMEM)] * 2 + [pl.BlockSpec(memory_space=pl.ANY)] * 5,
            out_specs=pl.BlockSpec(memory_space=pl.ANY),
            scratch_shapes=[
                pltpu.VMEM((STEPS * rows, width), jnp.bfloat16),
                pltpu.VMEM((rows, width), jnp.bfloat16),
                dma((chunks,)), dma((STEPS,)),
            ],
            compiler_params=pltpu.CompilerParams(vmem_limit_bytes=20 * 1024 * 1024),
        )(*results[:2], right, *results[2:])

    return jax.shard_map(
        local,
        mesh=mesh,
        in_specs=(P("row", "col"), P("row", "col")),
        out_specs=P("row", "col"),
        check_vma=False,
    )
```
